32 devices in a mesh: gx: 8 (over y, x, core), gy: 4 (over z).
Axes of the slice: x: 2, y: 2, z: 4, core: 2. Of those that a mesh axis runs over, the one named last changes fastest.
Arguments:
- east_class: int32 [512, 256], P('gx', 'gy'), may hold values from 0 to 7
- south_class: int32 [512, 256], P('gx', 'gy'), may hold values from 0 to 7
- cond_table: float32 [8], replicated, may hold values from 0.5 to 4
- leakage: float32 [512, 256], P('gx', 'gy'), may hold values from 0.1 to 1
- pad_mask: int32 [512, 256], P('gx', 'gy'), may hold values 0 or 1
- load_current: float32 [512, 256, 256], P('gx', 'gy'), may hold values from -24 to 24
Outputs:
- potential: float32 [512, 256, 256], P('gx', 'gy')
The draws below stay inside these ranges and needn't reach their ends.
All inputs are finite; a program needn't handle non-finite values. No bound on the sum of `pad_mask` on one device may be relied on, other than what follows from the above.
Results may differ from the reference program's by a relative error of at most 0.00002.
Values sent between devices are 32-bit elements; how exact they have to be, the bound alone decides.
A program may use at most 64 MiB of HBM per device.

```python
import math
import jax
import jax.numpy as jnp

CASES = 256
CLASSES = 8
ITERS = 4
NX = 512
NY = 256


def touch_ends(values, key, smallest, top_value):
    extent = values.shape
    spot = [jax.random.randint(jax.random.fold_in(key, axis), (), 0, extent[axis]) for axis in range(len(extent))]
    values = values.at[tuple(spot)].set(smallest)
    longest = extent.index(max(extent))
    spot[longest] = (spot[longest] + 1) % extent[longest]
    return values.at[tuple(spot)].set(top_value)


def shard_levels(stream_key, shape, pieces, smallest, high):
    gain, own = 1.0, jax.random.fold_in(stream_key, 6)
    for axis_at, shards_of in pieces:
        draws = jnp.exp(jax.random.uniform(jax.random.fold_in(own, axis_at), (shards_of,), jnp.float32, smallest / len(pieces), high / len(pieces)))
        gain = gain * jnp.repeat(draws, shape[axis_at] // shards_of).reshape([-1 if axis == axis_at else 1 for axis in range(len(shape))])
    return gain


def scatter_about(stream_key, dims, deviation, bound, split=(), kind=jnp.bfloat16):
    array = deviation * jax.random.normal(stream_key, dims, jnp.float32)
    if split:
        array = array * shard_levels(stream_key, dims, split, -0.22, 0.18)
    return jnp.clip(array, -bound, bound).astype(kind)


def setup_inputs(seed: int = 0) -> dict:
    streams_of = jax.random.split(jax.random.key(seed), 7)
    east_class = touch_ends(jax.random.randint(streams_of[0], (NX, NY), 0, CLASSES), jax.random.fold_in(streams_of[0], 1), 0, CLASSES - 1).astype(jnp.int32)
    south_class = touch_ends(jax.random.randint(streams_of[1], (NX, NY), 0, CLASSES), jax.random.fold_in(streams_of[1], 1), 0, CLASSES - 1).astype(jnp.int32)
    cond_table = jnp.clip(jnp.exp(jax.random.uniform(streams_of[2], (CLASSES,), jnp.float32, math.log(0.5), math.log(4.0))), 0.5, 4.0)
    leakage = jnp.clip(jnp.exp(math.log(1.0) - 2.3025851 * jax.random.uniform(streams_of[3], (NX, NY), jnp.float32) ** shard_levels(streams_of[3], (NX, NY), ((0, 8), (1, 4)), -0.2, 0.2)), 0.1, 1.0)
    pad_mask = touch_ends((jax.random.randint(streams_of[4], (NX, NY), 0, 8) < 1).astype(jnp.int32), jax.random.fold_in(streams_of[4], 1), 0, 1)
    load_current = scatter_about(streams_of[5], (NX, NY, CASES), 4.0, 24.0, ((0, 8), (1, 4)), jnp.float32)
    return dict(east_class=east_class, south_class=south_class, cond_table=cond_table, leakage=leakage, pad_mask=pad_mask, load_current=load_current)


PAD_GAIN = 8.0
SPECTRAL_BOUND = 0.995


def chebyshev_weights(total_steps):
    weights = [1.0]
    for position in range(1, total_steps):
        if position == 1:
            weights.append(1.0 / (1.0 - SPECTRAL_BOUND * SPECTRAL_BOUND / 2.0))
        else:
            weights.append(1.0 / (1.0 - SPECTRAL_BOUND * SPECTRAL_BOUND * weights[-1] / 4.0))
    return weights


def lookup(classes, cond_table):
    labels = jnp.arange(cond_table.shape[0], dtype=jnp.int32)
    matches = classes[:, :, None] == labels
    return jnp.sum(jnp.where(matches, cond_table, 0.0), axis=-1)


def reference(east_class, south_class, cond_table, leakage, pad_mask, load_current):
    east_cond = lookup(east_class, cond_table)
    south_cond = lookup(south_class, cond_table)
    pads = pad_mask.astype(jnp.float32)
    east_west = jnp.roll(east_cond, 1, 1)
    south_north = jnp.roll(south_cond, 1, 0)
    diagonal = east_cond + east_west + south_cond + south_north + (leakage + PAD_GAIN * pads)
    source = (PAD_GAIN * pads[:, :, None] - load_current) / diagonal[:, :, None]
    omegas = chebyshev_weights(ITERS)
    field = source
    previous = source
    for iteration in range(ITERS):
        neighbours = east_cond[:, :, None] * jnp.roll(field, -1, 1) + east_west[:, :, None] * jnp.roll(field, 1, 1)
        neighbours = neighbours + south_cond[:, :, None] * jnp.roll(field, -1, 0)
        neighbours = neighbours + south_north[:, :, None] * jnp.roll(field, 1, 0)
        jacobi_value = source + neighbours / diagonal[:, :, None]
        if iteration == 0:
            updated = jacobi_value
        else:
            updated = omegas[iteration] * (jacobi_value - previous) + previous
        previous, field = field, updated
    return field
```

```python
import functools

import jax
import jax.numpy as jnp
from jax import lax
from jax.experimental import pallas as pl
from jax.experimental.pallas import tpu as pltpu
from jax.sharding import PartitionSpec as P

ITERS = 4
PAD_GAIN = 8.0
SPECTRAL_BOUND = 0.995
G = ITERS
MESH = pl.DeviceIdType.MESH
CHUNKS = 2


def polynomial():
    weights = [1.0]
    for k in range(1, ITERS):
        if k == 1:
            weights.append(1.0 / (1.0 - SPECTRAL_BOUND**2 / 2.0))
        else:
            weights.append(1.0 / (1.0 - SPECTRAL_BOUND**2 * weights[-1] / 4.0))
    size = ITERS + 1
    previous = [1.0] + [0.0] * (size - 1)
    field = [1.0, 1.0] + [0.0] * (size - 2)
    for k in range(1, ITERS):
        jac = [1.0] + field[:-1]
        updated = [weights[k] * (a - b) + b for a, b in zip(jac, previous)]
        previous, field = field, updated
    return field


def kernel(
    nx, ny, rows, cols,
    table_ref, east_ref, south_ref, leak_ref, pad_ref, x_ref, o_ref,
    cf, tw, ew_src, ew_dst, load, src, v1, v2, v3, bc,
    eload, esrc, e1, e2, e3, ebc,
    local_sem, send_sem, recv_sem,
):
    mx, my = lax.axis_index("gx"), lax.axis_index("gy")
    north, south = lax.rem(mx + nx - 1, nx), lax.rem(mx + 1, nx)
    west, east = lax.rem(my + ny - 1, ny), lax.rem(my + 1, ny)
    cases = x_ref.shape[2]
    halves = [slice(h * 128, (h + 1) * 128) for h in range(cases // 128)]
    poly = polynomial()

    barrier = pltpu.get_barrier_semaphore()
    peers = [
        (north, my), (south, my), (mx, west), (mx, east),
        (north, west), (north, east), (south, west), (south, east),
    ]
    for peer in peers:
        pl.semaphore_signal(barrier, inc=1, device_id=peer, device_id_type=MESH)
    own = pltpu.make_async_copy(x_ref, load.at[pl.ds(G, rows)], local_sem)
    own.start()

    def lookup(classes):
        value = jnp.full(classes.shape, table_ref[0], jnp.float32)
        for c in range(1, table_ref.shape[0]):
            value = jnp.where(classes == c, table_ref[c], value)
        return value

    blank = jnp.zeros((rows, 128 - cols), jnp.float32)
    fields = [
        lookup(east_ref[...]),
        lookup(south_ref[...]),
        leak_ref[...] + PAD_GAIN * pad_ref[...].astype(jnp.float32),
    ]
    for f in range(3):
        cf[f, pl.ds(8, rows), :] = jnp.concatenate([fields[f], blank], axis=1)
    square = jnp.concatenate([fields[0], blank], axis=1)
    above, below = jnp.zeros((8, 128), jnp.float32), jnp.zeros((120 - rows, 128), jnp.float32)
    square = jnp.concatenate([above, square, below], axis=0)
    ew_src[...] = jnp.transpose(square)[cols - 8 : cols, :]

    pl.semaphore_wait(barrier, len(peers))

    counter = [0]

    def send(source, target, device):
        n = counter[0]
        counter[0] += 1
        copy = pltpu.make_async_remote_copy(
            src_ref=source, dst_ref=target,
            send_sem=send_sem.at[n], recv_sem=recv_sem.at[n],
            device_id=device, device_id_type=MESH,
        )
        copy.start()
        return copy

    cf_n = send(cf.at[:, pl.ds(rows, 8)], cf.at[:, pl.ds(0, 8)], (south, my))
    cf_s = send(cf.at[:, pl.ds(8, 8)], cf.at[:, pl.ds(rows + 8, 8)], (north, my))
    ew = send(ew_src, ew_dst, (mx, east))
    ld_n = send(x_ref.at[pl.ds(rows - G, G)], load.at[pl.ds(0, G)], (south, my))
    ld_s = send(x_ref.at[pl.ds(0, G)], load.at[pl.ds(rows + G, G)], (north, my))
    half = rows // CHUNKS
    low, high = pl.ds(0, G), pl.ds(cols - G, G)
    to_left, to_right = pl.ds(0, G), pl.ds(G, G)
    D = G - 1

    def side(start, count, at, row_from, vertical):
        return [
            send(
                x_ref.at[pl.ds(row_from, count), high],
                eload.at[0, pl.ds(at, count), to_left],
                (vertical, east),
            ),
            send(
                x_ref.at[pl.ds(row_from, count), low],
                eload.at[1, pl.ds(at, count), to_right],
                (vertical, west),
            ),
        ]

    first = side(0, half, G, 0, mx)
    first += side(0, D, G - D, rows - D, south)

    cf_n.wait_recv()
    cf_s.wait_recv()
    for f in range(3):
        tw[f, pl.ds(8, cols), :] = jnp.transpose(cf[f])[0:cols, :]
    tw_w = send(tw.at[:, pl.ds(cols, 8)], tw.at[:, pl.ds(0, 8)], (mx, east))
    tw_e = send(tw.at[:, pl.ds(8, 8)], tw.at[:, pl.ds(cols + 8, 8)], (mx, west))
    second = side(0, rows - half, G + half, half, mx)
    second += side(0, D, rows + G, 0, north)

    def coefficients(e, e_west, s, extra):
        s_north = pltpu.roll(s, 1, 1)
        rd = 1.0 / (e + e_west + s + s_north + extra)
        pads = jnp.where(extra > PAD_GAIN / 2, PAD_GAIN, 0.0)
        return [e * rd, e_west * rd, s * rd, s_north * rd, rd, pads * rd]

    def spread(values, put, lo, count):
        def one(r):
            for q, value in enumerate(values):
                lane = pltpu.roll(value, lax.rem(128 - (r + 8 - G), 128), 1)
                put(q, r, jnp.broadcast_to(lane[:, 0:1], value.shape))
        lax.fori_loop(lo, lo + count, lambda r, c: (one(r), c)[1], 0)

    def put_own(q, r, value):
        bc[q, r] = value

    ew.wait_recv()
    e_own = tw[0, pl.ds(8, cols), :]
    column = lax.broadcasted_iota(jnp.int32, (cols, 128), 0)
    e_first = jnp.broadcast_to(ew_dst[7:8, :], (cols, 128))
    e_west = jnp.where(column == 0, e_first, pltpu.roll(e_own, 1, 0))
    spread(
        coefficients(e_own, e_west, tw[1, pl.ds(8, cols), :], tw[2, pl.ds(8, cols), :]),
        put_own, G, rows,
    )

    def source(lo, count):
        def one(r, c):
            for h in halves:
                src[r, :, h] = bc[5, r] - load[r, :, h] * bc[4, r]
            return c
        lax.fori_loop(lo, lo + count, one, 0)

    chain = [src, v1, v2, v3]
    echain = [esrc, e1, e2, e3]

    def store(k, r, h, value):
        if k == ITERS:
            o_ref[r - G, :, h] = value
        else:
            chain[k][r, :, h] = value

    def step(k, lo, count):
        vin = chain[k - 1]

        def one(r, c):
            for h in halves:
                row = vin[r, :, h]
                total = bc[0, r] * pltpu.roll(row, cols - 1, 0)
                total += bc[1, r] * pltpu.roll(row, 1, 0)
                total += bc[2, r] * vin[r + 1, :, h]
                total += bc[3, r] * vin[r - 1, :, h]
                if k == 1:
                    total = total * poly[ITERS]
                store(k, r, h, total + poly[ITERS - k] * src[r, :, h])
            return c

        lax.fori_loop(lo, lo + count, one, 0)

    own.wait()
    source(G, rows)
    for k in range(1, ITERS + 1):
        step(k, G + k, rows - 2 * k)

    tw_w.wait_recv()
    tw_e.wait_recv()

    def wide(start, size):
        area = pl.ds(start, size)
        return coefficients(
            tw[0, area, :], tw[0, pl.ds(start - 1, size), :], tw[1, area, :], tw[2, area, :]
        )

    k_own = wide(8, cols)
    spread(k_own, put_own, 0, G)
    spread(k_own, put_own, rows + G, G)
    k_left, k_right = wide(8 - G, 2 * G), wide(8 + cols - G, 2 * G)

    def put_edge(w, q, r, value):
        ebc[w, q, r] = value

    spread(k_left, functools.partial(put_edge, 0), 0, rows + 2 * G)
    spread(k_right, functools.partial(put_edge, 1), 0, rows + 2 * G)
    ld_n.wait_recv()
    ld_s.wait_recv()
    source(0, G)
    source(rows + G, G)
    for k in range(1, ITERS + 1):
        step(k, k, G)
        step(k, rows + 2 * G - k - G, G)

    lane_row = lax.broadcasted_iota(jnp.int32, (2 * G, 128), 0)
    tiles = [pl.ds(0, 2 * G), pl.ds(cols - 2 * G, 2 * G)]

    def edge_source(lo, count):
        def one(r, c):
            for h in halves:
                for w in range(2):
                    ghost = ebc[w, 5, r] - eload[w, r, :, h] * ebc[w, 4, r]
                    mine = pltpu.roll(src[r, tiles[w], h], G, 0)
                    keep = lane_row < G if w == 0 else lane_row >= G
                    esrc[w, r, :, h] = jnp.where(keep, ghost, mine)
            return c
        lax.fori_loop(lo, lo + count, one, 0)

    def edge_step(k, lo, count):
        vin, base = echain[k - 1], chain[k - 1]

        def one(r, c):
            for h in halves:
                for w in range(2):
                    row = vin[w, r, :, h]
                    inner = base[r, tiles[w], h]
                    to_east, to_west = pltpu.roll(row, 2 * G - 1, 0), pltpu.roll(row, 1, 0)
                    if w == 0:
                        to_east = jnp.where(lane_row == 2 * G - 1, pltpu.roll(inner, G - 1, 0), to_east)
                    else:
                        to_west = jnp.where(lane_row == 0, pltpu.roll(inner, G + 1, 0), to_west)
                    total = ebc[w, 0, r] * to_east + ebc[w, 1, r] * to_west
                    total += ebc[w, 2, r] * vin[w, r + 1, :, h]
                    total += ebc[w, 3, r] * vin[w, r - 1, :, h]
                    if k == 1:
                        total = total * poly[ITERS]
                    total += poly[ITERS - k] * esrc[w, r, :, h]
                    if k < ITERS:
                        echain[k][w, r, :, h] = total
                    else:
                        keep = lane_row < G if w == 0 else lane_row >= G
                        mixed = jnp.where(keep, pltpu.roll(total, G, 0), o_ref[r - G, tiles[w], h])
                        o_ref[r - G, tiles[w], h] = mixed
            return c

        lax.fori_loop(lo, lo + count, one, 0)

    for copy in first:
        copy.wait_recv()
    cut = G + half
    edge_source(0, cut)
    for k in range(1, ITERS + 1):
        edge_step(k, k, cut - 2 * k)
    for copy in second:
        copy.wait_recv()
    edge_source(cut, rows + 2 * G - cut)
    for k in range(1, ITERS + 1):
        edge_step(k, cut - k, rows + 2 * G - cut)
    for copy in [cf_n, cf_s, ew, ld_n, ld_s, tw_w, tw_e] + first + second:
        copy.wait_send()


def body(nx, ny, east_class, south_class, cond_table, leakage, pad_mask, load_current):
    rows, cols, cases = load_current.shape
    tall = rows + 2 * G
    f32 = jnp.float32
    vmem = pl.BlockSpec(memory_space=pltpu.VMEM)
    copies = 7 + 8
    return pl.pallas_call(
        functools.partial(kernel, nx, ny, rows, cols),
        out_shape=jax.ShapeDtypeStruct(load_current.shape, f32),
        in_specs=[pl.BlockSpec(memory_space=pltpu.SMEM), vmem, vmem, vmem, vmem,
                  pl.BlockSpec(memory_space=pl.ANY)],
        out_specs=vmem,
        scratch_shapes=[
            pltpu.VMEM((3, 128, 128), f32),
            pltpu.VMEM((3, cols + 16, 128), f32),
            pltpu.VMEM((8, 128), f32),
            pltpu.VMEM((8, 128), f32),
            pltpu.VMEM((tall, cols, cases), f32),
            pltpu.VMEM((tall, cols, cases), f32),
            pltpu.VMEM((tall, cols, cases), f32),
            pltpu.VMEM((tall, cols, cases), f32),
            pltpu.VMEM((tall, cols, cases), f32),
            pltpu.VMEM((6, tall, cols, 128), f32),
            pltpu.VMEM((2, tall, 2 * G, cases), f32),
            pltpu.VMEM((2, tall, 2 * G, cases), f32),
            pltpu.VMEM((2, tall, 2 * G, cases), f32),
            pltpu.VMEM((2, tall, 2 * G, cases), f32),
            pltpu.VMEM((2, tall, 2 * G, cases), f32),
            pltpu.VMEM((2, 6, tall, 2 * G, 128), f32),
            pltpu.SemaphoreType.DMA,
            pltpu.SemaphoreType.DMA((copies,)),
            pltpu.SemaphoreType.DMA((copies,)),
        ],
        compiler_params=pltpu.CompilerParams(
            collective_id=0, has_side_effects=True, vmem_limit_bytes=67043328,
        ),
    )(cond_table, east_class, south_class, leakage, pad_mask, load_current)


def solution(mesh):
    in_specs = (
        P("gx", "gy"),
        P("gx", "gy"),
        P(),
        P("gx", "gy"),
        P("gx", "gy"),
        P("gx", "gy", None),
    )
    out_specs = P("gx", "gy", None)
    call = functools.partial(body, mesh.shape["gx"], mesh.shape["gy"])
    return jax.shard_map(call, mesh=mesh, in_specs=in_specs, out_specs=out_specs, check_vma=False)
```

```python
import functools

import jax
import jax.numpy as jnp
from jax import lax
from jax.experimental import pallas as pl
from jax.experimental.pallas import tpu as pltpu
from jax.sharding import PartitionSpec as P

ITERS = 4
PAD_GAIN = 8.0
SPECTRAL_BOUND = 0.995
G = ITERS
MESH = pl.DeviceIdType.MESH
CHUNKS = 2


def polynomial():
    weights = [1.0]
    for k in range(1, ITERS):
        if k == 1:
            weights.append(1.0 / (1.0 - SPECTRAL_BOUND**2 / 2.0))
        else:
            weights.append(1.0 / (1.0 - SPECTRAL_BOUND**2 * weights[-1] / 4.0))
    size = ITERS + 1
    previous = [1.0] + [0.0] * (size - 1)
    field = [1.0, 1.0] + [0.0] * (size - 2)
    for k in range(1, ITERS):
        jac = [1.0] + field[:-1]
        updated = [weights[k] * (a - b) + b for a, b in zip(jac, previous)]
        previous, field = field, updated
    return field


def loop(lo, count, width, compute):
    def turn(start, size):
        pending = [compute(start + u) for u in range(size)]
        for stores in pending:
            for put in stores:
                put()

    turns, rest = count // width, count % width
    if turns:
        lax.fori_loop(0, turns, lambda t, c: (turn(lo + t * width, width), c)[1], 0)
    if rest:
        turn(lo + turns * width, rest)


def setter(ref, index, value):
    def put():
        ref[index] = value
    return put


def kernel(
    nx, ny, rows, cols,
    table_ref, east_ref, south_ref, leak_ref, pad_ref, x_ref, o_ref,
    cf, tw, ew_src, ew_dst, load, src, v1, v2, v3, bc,
    eload, esrc, e1, e2, e3, ebc,
    local_sem, send_sem, recv_sem,
):
    mx, my = lax.axis_index("gx"), lax.axis_index("gy")
    north, south = lax.rem(mx + nx - 1, nx), lax.rem(mx + 1, nx)
    west, east = lax.rem(my + ny - 1, ny), lax.rem(my + 1, ny)
    cases = x_ref.shape[2]
    halves = [slice(h * 128, (h + 1) * 128) for h in range(cases // 128)]
    poly = polynomial()

    barrier = pltpu.get_barrier_semaphore()
    peers = [(north, my), (south, my), (mx, west), (mx, east)]
    for peer in peers:
        pl.semaphore_signal(barrier, inc=1, device_id=peer, device_id_type=MESH)
    own = pltpu.make_async_copy(x_ref, load.at[pl.ds(G, rows)], local_sem)
    own.start()

    def lookup(classes):
        value = jnp.full(classes.shape, table_ref[0], jnp.float32)
        for c in range(1, table_ref.shape[0]):
            value = jnp.where(classes == c, table_ref[c], value)
        return value

    blank = jnp.zeros((rows, 128 - cols), jnp.float32)
    fields = [
        lookup(east_ref[...]),
        lookup(south_ref[...]),
        leak_ref[...] + PAD_GAIN * pad_ref[...].astype(jnp.float32),
    ]
    for f in range(3):
        cf[f, pl.ds(8, rows), :] = jnp.concatenate([fields[f], blank], axis=1)
    square = jnp.concatenate([fields[0], blank], axis=1)
    above, below = jnp.zeros((8, 128), jnp.float32), jnp.zeros((120 - rows, 128), jnp.float32)
    square = jnp.concatenate([above, square, below], axis=0)
    ew_src[...] = jnp.transpose(square)[cols - 8 : cols, :]

    pl.semaphore_wait(barrier, len(peers))

    counter = [0]

    def send(source, target, device):
        n = counter[0]
        counter[0] += 1
        copy = pltpu.make_async_remote_copy(
            src_ref=source, dst_ref=target,
            send_sem=send_sem.at[n], recv_sem=recv_sem.at[n],
            device_id=device, device_id_type=MESH,
        )
        copy.start()
        return copy

    cf_n = send(cf.at[:, pl.ds(rows, 8)], cf.at[:, pl.ds(0, 8)], (south, my))
    cf_s = send(cf.at[:, pl.ds(8, 8)], cf.at[:, pl.ds(rows + 8, 8)], (north, my))
    ew = send(ew_src, ew_dst, (mx, east))
    ld_n = send(x_ref.at[pl.ds(rows - G, G)], load.at[pl.ds(0, G)], (south, my))
    ld_s = send(x_ref.at[pl.ds(0, G)], load.at[pl.ds(rows + G, G)], (north, my))
    half = rows // CHUNKS
    low, high = pl.ds(0, G), pl.ds(cols - G, G)
    to_left, to_right = pl.ds(0, G), pl.ds(G, G)
    D = G - 1

    def side(count, at, ref, row_from):
        return [
            send(
                ref.at[pl.ds(row_from, count), high],
                eload.at[0, pl.ds(at, count), to_left],
                (mx, east),
            ),
            send(
                ref.at[pl.ds(row_from, count), low],
                eload.at[1, pl.ds(at, count), to_right],
                (mx, west),
            ),
        ]

    first = side(half, G, x_ref, 0)

    cf_n.wait_recv()
    cf_s.wait_recv()
    for f in range(3):
        tw[f, pl.ds(8, cols), :] = jnp.transpose(cf[f])[0:cols, :]
    tw_w = send(tw.at[:, pl.ds(cols, 8)], tw.at[:, pl.ds(0, 8)], (mx, east))
    tw_e = send(tw.at[:, pl.ds(8, 8)], tw.at[:, pl.ds(cols + 8, 8)], (mx, west))
    second = side(rows - half, G + half, x_ref, half)

    def coefficients(e, e_west, s, extra):
        s_north = pltpu.roll(s, 1, 1)
        rd = 1.0 / (e + e_west + s + s_north + extra)
        pads = jnp.where(extra > PAD_GAIN / 2, PAD_GAIN, 0.0)
        return [e * rd, e_west * rd, s * rd, s_north * rd, rd, pads * rd]

    def spread(values, put, lo, count, width):
        def block(t):
            r = lo + t * width
            for q, value in enumerate(values):
                rolled = pltpu.roll(value, 128 - (r + 8 - G), 1)
                for u in range(width):
                    put(q, r + u, jnp.broadcast_to(rolled[:, u : u + 1], value.shape))
        lax.fori_loop(0, count // width, lambda t, c: (block(t), c)[1], 0)

    def put_own(q, r, value):
        bc[q, r] = value

    ew.wait_recv()
    e_own = tw[0, pl.ds(8, cols), :]
    column = lax.broadcasted_iota(jnp.int32, (cols, 128), 0)
    e_first = jnp.broadcast_to(ew_dst[7:8, :], (cols, 128))
    e_west = jnp.where(column == 0, e_first, pltpu.roll(e_own, 1, 0))
    spread(
        coefficients(e_own, e_west, tw[1, pl.ds(8, cols), :], tw[2, pl.ds(8, cols), :]),
        put_own, G, rows, 8,
    )

    def source(lo, count):
        def one(r):
            return [
                setter(src, (r, slice(None), h), bc[5, r] - load[r, :, h] * bc[4, r])
                for h in halves
            ]
        loop(lo, count, 2, one)

    chain = [src, v1, v2, v3]
    echain = [esrc, e1, e2, e3]

    def step(k, lo, count):
        vin = chain[k - 1]

        def one(r):
            stores = []
            for h in halves:
                row = vin[r, :, h]
                total = bc[0, r] * pltpu.roll(row, cols - 1, 0)
                total += bc[1, r] * pltpu.roll(row, 1, 0)
                total += bc[2, r] * vin[r + 1, :, h]
                total += bc[3, r] * vin[r - 1, :, h]
                if k == 1:
                    total = total * poly[ITERS]
                total += poly[ITERS - k] * src[r, :, h]
                out, at = (o_ref, r - G) if k == ITERS else (chain[k], r)
                stores.append(setter(out, (at, slice(None), h), total))
            return stores

        loop(lo, count, 2, one)

    own.wait()
    source(G, rows)
    step(1, G + 1, rows - 2)

    ld_n.wait_recv()
    ld_s.wait_recv()
    first += side(D, G - D, load, G - D)
    second += side(D, rows + G, load, rows + G)
    for k in range(2, ITERS + 1):
        step(k, G + k, rows - 2 * k)

    tw_w.wait_recv()
    tw_e.wait_recv()

    def wide(start, size):
        area = pl.ds(start, size)
        return coefficients(
            tw[0, area, :], tw[0, pl.ds(start - 1, size), :], tw[1, area, :], tw[2, area, :]
        )

    k_own = wide(8, cols)
    spread(k_own, put_own, 0, G, G)
    spread(k_own, put_own, rows + G, G, G)
    k_left, k_right = wide(8 - G, 2 * G), wide(8 + cols - G, 2 * G)

    def put_edge(w, q, r, value):
        ebc[w, q, r] = value

    spread(k_left, functools.partial(put_edge, 0), 0, rows + 2 * G, 8)
    spread(k_right, functools.partial(put_edge, 1), 0, rows + 2 * G, 8)
    source(0, G)
    source(rows + G, G)
    for k in range(1, ITERS + 1):
        step(k, k, G)
        step(k, rows + 2 * G - k - G, G)

    lane_row = lax.broadcasted_iota(jnp.int32, (2 * G, 128), 0)
    tiles = [pl.ds(0, 2 * G), pl.ds(cols - 2 * G, 2 * G)]

    def edge_source(lo, count):
        def one(r):
            stores = []
            for h in halves:
                for w in range(2):
                    ghost = ebc[w, 5, r] - eload[w, r, :, h] * ebc[w, 4, r]
                    mine = pltpu.roll(src[r, tiles[w], h], G, 0)
                    keep = lane_row < G if w == 0 else lane_row >= G
                    stores.append(setter(esrc, (w, r, slice(None), h), jnp.where(keep, ghost, mine)))
            return stores
        loop(lo, count, 4, one)

    def edge_step(k, lo, count):
        vin, base = echain[k - 1], chain[k - 1]

        def one(r):
            stores = []
            for h in halves:
                for w in range(2):
                    row = vin[w, r, :, h]
                    inner = base[r, tiles[w], h]
                    to_east, to_west = pltpu.roll(row, 2 * G - 1, 0), pltpu.roll(row, 1, 0)
                    if w == 0:
                        to_east = jnp.where(lane_row == 2 * G - 1, pltpu.roll(inner, G - 1, 0), to_east)
                    else:
                        to_west = jnp.where(lane_row == 0, pltpu.roll(inner, G + 1, 0), to_west)
                    total = ebc[w, 0, r] * to_east + ebc[w, 1, r] * to_west
                    total += ebc[w, 2, r] * vin[w, r + 1, :, h]
                    total += ebc[w, 3, r] * vin[w, r - 1, :, h]
                    if k == 1:
                        total = total * poly[ITERS]
                    total += poly[ITERS - k] * esrc[w, r, :, h]
                    if k < ITERS:
                        stores.append(setter(echain[k], (w, r, slice(None), h), total))
                    else:
                        keep = lane_row < G if w == 0 else lane_row >= G
                        mixed = jnp.where(keep, pltpu.roll(total, G, 0), o_ref[r - G, tiles[w], h])
                        stores.append(setter(o_ref, (r - G, tiles[w], h), mixed))
            return stores

        loop(lo, count, 4, one)

    for copy in first:
        copy.wait_recv()
    cut = G + half
    edge_source(0, cut)
    for k in range(1, ITERS + 1):
        edge_step(k, k, cut - 2 * k)
    for copy in second:
        copy.wait_recv()
    edge_source(cut, rows + 2 * G - cut)
    for k in range(1, ITERS + 1):
        edge_step(k, cut - k, rows + 2 * G - cut)
    for copy in [cf_n, cf_s, ew, ld_n, ld_s, tw_w, tw_e] + first + second:
        copy.wait_send()


def body(nx, ny, east_class, south_class, cond_table, leakage, pad_mask, load_current):
    rows, cols, cases = load_current.shape
    tall = rows + 2 * G
    f32 = jnp.float32
    vmem = pl.BlockSpec(memory_space=pltpu.VMEM)
    copies = 7 + 8
    return pl.pallas_call(
        functools.partial(kernel, nx, ny, rows, cols),
        out_shape=pltpu.VMEM(load_current.shape, f32),
        in_specs=[pl.BlockSpec(memory_space=pltpu.SMEM), vmem, vmem, vmem, vmem,
                  pl.BlockSpec(memory_space=pl.ANY)],
        out_specs=vmem,
        scratch_shapes=[
            pltpu.VMEM((3, 128, 128), f32),
            pltpu.VMEM((3, cols + 16, 128), f32),
            pltpu.VMEM((8, 128), f32),
            pltpu.VMEM((8, 128), f32),
            pltpu.VMEM((tall, cols, cases), f32),
            pltpu.VMEM((tall, cols, cases), f32),
            pltpu.VMEM((tall, cols, cases), f32),
            pltpu.VMEM((tall, cols, cases), f32),
            pltpu.VMEM((tall, cols, cases), f32),
            pltpu.VMEM((6, tall, cols, 128), f32),
            pltpu.VMEM((2, tall, 2 * G, cases), f32),
            pltpu.VMEM((2, tall, 2 * G, cases), f32),
            pltpu.VMEM((2, tall, 2 * G, cases), f32),
            pltpu.VMEM((2, tall, 2 * G, cases), f32),
            pltpu.VMEM((2, tall, 2 * G, cases), f32),
            pltpu.VMEM((2, 6, tall, 2 * G, 128), f32),
            pltpu.SemaphoreType.DMA,
            pltpu.SemaphoreType.DMA((copies,)),
            pltpu.SemaphoreType.DMA((copies,)),
        ],
        compiler_params=pltpu.CompilerParams(
            collective_id=0, has_side_effects=True, vmem_limit_bytes=57 * 2**20,
        ),
    )(cond_table, east_class, south_class, leakage, pad_mask, load_current)


def solution(mesh):
    in_specs = (
        P("gx", "gy"),
        P("gx", "gy"),
        P(),
        P("gx", "gy"),
        P("gx", "gy"),
        P("gx", "gy", None),
    )
    out_specs = P("gx", "gy", None)
    call = functools.partial(body, mesh.shape["gx"], mesh.shape["gy"])
    return jax.shard_map(call, mesh=mesh, in_specs=in_specs, out_specs=out_specs, check_vma=False)
```

```python
import functools

import jax
import jax.numpy as jnp
from jax import lax
from jax.experimental import pallas as pl
from jax.experimental.pallas import tpu as pltpu
from jax.sharding import PartitionSpec as P

ITERS = 4
PAD_GAIN = 8.0
SPECTRAL_BOUND = 0.995
G = ITERS
MESH = pl.DeviceIdType.MESH
CHUNKS = 2


def polynomial():
    weights = [1.0]
    for k in range(1, ITERS):
        if k == 1:
            weights.append(1.0 / (1.0 - SPECTRAL_BOUND**2 / 2.0))
        else:
            weights.append(1.0 / (1.0 - SPECTRAL_BOUND**2 * weights[-1] / 4.0))
    size = ITERS + 1
    previous = [1.0] + [0.0] * (size - 1)
    field = [1.0, 1.0] + [0.0] * (size - 2)
    for k in range(1, ITERS):
        jac = [1.0] + field[:-1]
        updated = [weights[k] * (a - b) + b for a, b in zip(jac, previous)]
        previous, field = field, updated
    return field


def loop(lo, count, width, compute):
    def turn(start, size):
        pending = [compute(start + u) for u in range(size)]
        for stores in pending:
            for put in stores:
                put()

    turns, rest = count // width, count % width
    if turns:
        lax.fori_loop(0, turns, lambda t, c: (turn(lo + t * width, width), c)[1], 0)
    if rest:
        turn(lo + turns * width, rest)


def setter(ref, index, value):
    def put():
        ref[index] = value
    return put


def kernel(
    nx, ny, rows, cols,
    table_ref, east_ref, south_ref, leak_ref, pad_ref, x_ref, o_ref,
    cf, tw, load, src, v1, v2, v3, bc,
    eload, west_bc, east_bc,
    local_sem, send_sem, recv_sem,
):
    mx, my = lax.axis_index("gx"), lax.axis_index("gy")
    north, south = lax.rem(mx + nx - 1, nx), lax.rem(mx + 1, nx)
    west, east = lax.rem(my + ny - 1, ny), lax.rem(my + 1, ny)
    cases = x_ref.shape[2]
    halves = [slice(h * 128, (h + 1) * 128) for h in range(cases // 128)]
    poly = polynomial()

    barrier = pltpu.get_barrier_semaphore()
    peers = [(north, my), (south, my), (mx, west), (mx, east)]
    for peer in peers:
        pl.semaphore_signal(barrier, inc=1, device_id=peer, device_id_type=MESH)
    own = pltpu.make_async_copy(x_ref, load.at[pl.ds(G, rows)], local_sem)
    own.start()

    def lookup(classes):
        value = jnp.full(classes.shape, table_ref[0], jnp.float32)
        for c in range(1, table_ref.shape[0]):
            value = jnp.where(classes == c, table_ref[c], value)
        return value

    blank = jnp.zeros((rows, 128 - cols), jnp.float32)
    fields = [
        lookup(east_ref[...]),
        lookup(south_ref[...]),
        leak_ref[...] + PAD_GAIN * pad_ref[...].astype(jnp.float32),
    ]
    for f in range(3):
        cf[f, pl.ds(8, rows), :] = jnp.concatenate([fields[f], blank], axis=1)
    above, below = jnp.zeros((8, 128), jnp.float32), jnp.zeros((120 - rows, 128), jnp.float32)
    for f in range(3):
        square = jnp.concatenate([above, jnp.concatenate([fields[f], blank], axis=1), below], axis=0)
        tw[f, pl.ds(8, cols), :] = jnp.transpose(square)[0:cols, :]

    pl.semaphore_wait(barrier, len(peers))

    counter = [0]

    def send(source, target, device):
        n = counter[0]
        counter[0] += 1
        copy = pltpu.make_async_remote_copy(
            src_ref=source, dst_ref=target,
            send_sem=send_sem.at[n], recv_sem=recv_sem.at[n],
            device_id=device, device_id_type=MESH,
        )
        copy.start()
        return copy

    cf_n = send(cf.at[:, pl.ds(rows, 8)], cf.at[:, pl.ds(0, 8)], (south, my))
    cf_s = send(cf.at[:, pl.ds(8, 8)], cf.at[:, pl.ds(rows + 8, 8)], (north, my))
    ld_n = send(x_ref.at[pl.ds(rows - G, G)], load.at[pl.ds(0, G)], (south, my))
    ld_s = send(x_ref.at[pl.ds(0, G)], load.at[pl.ds(rows + G, G)], (north, my))
    half = rows // CHUNKS
    low, high = pl.ds(0, G), pl.ds(cols - G, G)
    to_left, to_right = pl.ds(0, G), pl.ds(G, G)
    D = G - 1

    def side(count, at, ref, row_from):
        return [
            send(
                ref.at[pl.ds(row_from, count), high],
                eload.at[0, pl.ds(at, count), to_left],
                (mx, east),
            ),
            send(
                ref.at[pl.ds(row_from, count), low],
                eload.at[1, pl.ds(at, count), to_right],
                (mx, west),
            ),
        ]

    first = side(half, G, x_ref, 0)

    def ratios(e, e_west, s, s_north, extra):
        rd = 1.0 / (e + e_west + s + s_north + extra)
        pads = jnp.where(extra > PAD_GAIN / 2, PAD_GAIN, 0.0)
        return [e * rd, e_west * rd, s * rd, s_north * rd, rd, pads * rd]

    def spread(e, s, extra, before, put, lo, count, width):
        size = e.shape[0]
        first = lax.broadcasted_iota(jnp.int32, (size, 128), 0) == 0

        def block(t):
            r = lo + t * width
            amount = 128 - (r + 8 - G)
            e_at, s_at, x_at = (pltpu.roll(value, amount, 1) for value in (e, s, extra))
            w_at = pltpu.roll(before, amount, 1)
            over = lambda value, u: jnp.broadcast_to(value[:, u : u + 1], (value.shape[0], 128))
            s_north = over(s_at, 127)
            for u in range(width):
                e_now, s_now = over(e_at, u), over(s_at, u)
                head = jnp.broadcast_to(over(w_at, u)[7:8, :], (size, 128))
                e_west = jnp.where(first, head, pltpu.roll(e_now, 1, 0))
                for q, value in enumerate(ratios(e_now, e_west, s_now, s_north, over(x_at, u))):
                    put(q, r + u, value)
                s_north = s_now
        lax.fori_loop(0, count // width, lambda t, c: (block(t), c)[1], 0)

    def put_own(q, r, value):
        bc[q, r] = value

    area = pl.ds(8, cols)
    own_fields = [tw[f, area, :] for f in range(3)]
    spread(*own_fields, tw[0, area, :][0:8], put_own, G, rows, 8)

    cf_n.wait_recv()
    cf_s.wait_recv()
    for f in range(3):
        tw[f, pl.ds(8, cols), :] = jnp.transpose(cf[f])[0:cols, :]
    tw_w = send(tw.at[:, pl.ds(cols, 8)], tw.at[:, pl.ds(0, 8)], (mx, east))
    tw_e = send(tw.at[:, pl.ds(8, 8)], tw.at[:, pl.ds(cols + 8, 8)], (mx, west))
    second = side(rows - half, G + half, x_ref, half)

    chain = [src, v1, v2, v3]

    def source(lo, count):
        def one(r):
            return [
                setter(src, (r, n, pl.ds(8, cols)), bc[5, r] - load[r, :, h] * bc[4, r])
                for n, h in enumerate(halves)
            ]
        loop(lo, count, 2, one)

    def update(k, r, n, at, size, coefs):
        vin = chain[k - 1]
        total = coefs[0] * vin[r, n, pl.ds(at + 1, size)]
        total += coefs[1] * vin[r, n, pl.ds(at - 1, size)]
        total += coefs[2] * vin[r + 1, n, pl.ds(at, size)]
        total += coefs[3] * vin[r - 1, n, pl.ds(at, size)]
        if k == 1:
            total = total * poly[ITERS]
        return total + poly[ITERS - k] * src[r, n, pl.ds(at, size)]

    def step(k, lo, count):
        def one(r):
            stores = []
            coefs = [bc[q, r] for q in range(4)]
            for n, h in enumerate(halves):
                total = update(k, r, n, 8, cols, coefs)
                if k == ITERS:
                    stores.append(setter(o_ref, (r - G, slice(None), h), total))
                else:
                    stores.append(setter(chain[k], (r, n, pl.ds(8, cols)), total))
            return stores

        loop(lo, count, 2, one)

    own.wait()
    source(G, rows)
    step(1, G + 2, rows - 3)

    ld_n.wait_recv()
    ld_s.wait_recv()
    first += side(D, G - D, load, G - D)
    second += side(D, rows + G, load, rows + G)
    for k in range(2, ITERS + 1):
        step(k, G + k + 1, rows - 2 * k - 1)

    tw_w.wait_recv()
    tw_e.wait_recv()

    def put_edge(w, q, r, value):
        (west_bc, east_bc)[w][q, r] = value

    def wide(start, size, *rest):
        fields = [tw[f, pl.ds(start, size), :] for f in range(3)]
        row = tw[0, pl.ds(max(start - 1, 0), 1), :]
        spread(*fields, jnp.broadcast_to(row, (8, 128)), *rest)

    wide(8, cols, put_own, 0, G + 1, G + 1)
    wide(8, cols, put_own, rows + G, G, G)
    wide(0, 16, functools.partial(put_edge, 0), 0, rows + 2 * G, 8)
    wide(8 + cols - G, 2 * G, functools.partial(put_edge, 1), 0, rows + 2 * G, 8)
    source(0, G + 1)
    source(rows + G, G)
    for k in range(1, ITERS + 1):
        step(k, k, G + 1)
        step(k, rows + 2 * G - k - G, G)

    lane_row = lax.broadcasted_iota(jnp.int32, (2 * G, 128), 0)
    starts = [9 - G, 8 + cols - G]
    tiles = [pl.ds(start, 2 * G) for start in starts]
    ghosts = [pl.ds(8 - G, 2 * G), tiles[1]]
    mine = [pl.ds(0, G + 1), pl.ds(cols - G, G)]
    inner = [slice(G - 1, 2 * G), slice(0, G)]
    west_at = [pl.ds(9 - G, 2 * G)] * 4 + [pl.ds(8 - G, 2 * G)] * 2

    def edge_coef(w, q, r):
        return east_bc[q, r] if w else west_bc[q, r, west_at[q]]

    def edge_source(lo, count):
        def one(r):
            stores = []
            for n, h in enumerate(halves):
                near = pltpu.roll(load[r, pl.ds(0, 2 * G), h], G, 0)
                far = pltpu.roll(load[r, pl.ds(cols - 2 * G, 2 * G), h], G, 0)
                for w in range(2):
                    ghost = lane_row < G if w == 0 else lane_row >= G
                    full = jnp.where(ghost, eload[w, r, :, h], far if w else near)
                    value = edge_coef(w, 5, r) - full * edge_coef(w, 4, r)
                    stores.append(setter(src, (r, n, ghosts[w]), value))
            return stores
        loop(lo, count, 4, one)

    def edge_step(k, lo, count):
        def one(r):
            stores = []
            for w in range(2):
                coefs = [edge_coef(w, q, r) for q in range(4)]
                for n, h in enumerate(halves):
                    total = update(k, r, n, starts[w], 2 * G, coefs)
                    if k < ITERS:
                        stores.append(setter(chain[k], (r, n, tiles[w]), total))
                    else:
                        stores.append(setter(o_ref, (r - G, mine[w], h), total[inner[w]]))
            return stores

        loop(lo, count, 4, one)

    for copy in first:
        copy.wait_recv()
    cut = G + half
    edge_source(0, cut)
    for k in range(1, ITERS + 1):
        edge_step(k, k, cut - 2 * k)
    for copy in second:
        copy.wait_recv()
    edge_source(cut, rows + 2 * G - cut)
    for k in range(1, ITERS + 1):
        edge_step(k, cut - k, rows + 2 * G - cut)
    for copy in [cf_n, cf_s, ld_n, ld_s, tw_w, tw_e] + first + second:
        copy.wait_send()


def body(nx, ny, east_class, south_class, cond_table, leakage, pad_mask, load_current):
    rows, cols, cases = load_current.shape
    tall = rows + 2 * G
    f32 = jnp.float32
    vmem = pl.BlockSpec(memory_space=pltpu.VMEM)
    copies = 6 + 8
    return pl.pallas_call(
        functools.partial(kernel, nx, ny, rows, cols),
        out_shape=pltpu.VMEM(load_current.shape, f32),
        in_specs=[pl.BlockSpec(memory_space=pltpu.SMEM), vmem, vmem, vmem, vmem,
                  pl.BlockSpec(memory_space=pl.ANY)],
        out_specs=vmem,
        scratch_shapes=[
            pltpu.VMEM((3, 128, 128), f32),
            pltpu.VMEM((3, cols + 16, 128), f32),
            pltpu.VMEM((tall, cols, cases), f32),
            pltpu.VMEM((tall, cases // 128, cols + 16, 128), f32),
            pltpu.VMEM((tall, cases // 128, cols + 16, 128), f32),
            pltpu.VMEM((tall, cases // 128, cols + 16, 128), f32),
            pltpu.VMEM((tall, cases // 128, cols + 16, 128), f32),
            pltpu.VMEM((6, tall, cols, 128), f32),
            pltpu.VMEM((2, tall, 2 * G, cases), f32),
            pltpu.VMEM((6, tall, 16, 128), f32),
            pltpu.VMEM((6, tall, 2 * G, 128), f32),
            pltpu.SemaphoreType.DMA,
            pltpu.SemaphoreType.DMA((copies,)),
            pltpu.SemaphoreType.DMA((copies,)),
        ],
        compiler_params=pltpu.CompilerParams(
            collective_id=0, has_side_effects=True, vmem_limit_bytes=57 * 2**20,
        ),
    )(cond_table, east_class, south_class, leakage, pad_mask, load_current)


def solution(mesh):
    in_specs = (
        P("gx", "gy"),
        P("gx", "gy"),
        P(),
        P("gx", "gy"),
        P("gx", "gy"),
        P("gx", "gy", None),
    )
    out_specs = P("gx", "gy", None)
    call = functools.partial(body, mesh.shape["gx"], mesh.shape["gy"])
    return jax.shard_map(call, mesh=mesh, in_specs=in_specs, out_specs=out_specs, check_vma=False)
```
